32 devices in a mesh: grp: 8 (over y, x, core), blk: 4 (over z).
Axes of the slice: x: 2, y: 2, z: 4, core: 2. Of those that a mesh axis runs over, the one named last changes fastest.
Arguments:
- visual: bfloat16 [24576, 3584], P(('grp', 'blk')), may hold values from -6 to 6
- text_queries: float32 [1024, 3584], P(('grp', 'blk')), may hold values from -100 to 100
- kv_weight: bfloat16 [3584, 1024], replicated, may hold values from -0.09375 to 0.09375
- placement: int32 [3072, 1], P(('grp', 'blk')), may hold values from 0 to 31; in each aligned block of 96 rows (0 to 95, 96 to 191, ...) at most 4 rows name the same one
Outputs:
- attended: float32 [1024, 3584], P(('grp', 'blk'))
The draws below stay inside these ranges and needn't reach their ends.
Inputs may be any that keep to these rules, and one draw needn't show every extreme that they name: `placement`: among the 96 blocks of one frame owner at most 4 name the same attention owner, a bound that some block reaches; every attention owner is named by some block.
All inputs are finite; a program needn't handle non-finite values.
Results may differ from the reference program's by a relative error of at most 0.0003.
Values sent between devices are 32-bit elements; how exact they have to be, the bound alone decides.
A program may use at most 128 MiB of HBM per device.

```python
import math
import jax
import jax.numpy as jnp
import numpy as np
from jax import lax

DV = 3584
HEADS = 28
KV_HEADS = 4
HEAD_DIM = 128
QROWS = 32
BLOCKS = 96
BLOCK_ROWS = 8
PER_PAIR = 4
TEXT = 1024
VISUAL = 24576
N_GRP = 8
N_BLK = 4
DEVICES = 32


def draw_text_queries(key, part):
    base = jax.random.normal(key, (TEXT, HEADS * HEAD_DIM), jnp.float32)
    return jnp.clip(base, -100.0, 100.0)


def shard_levels(rng, shape, cuts, smallest, largest):
    gain = 1.0
    for dim, blocks in cuts:
        draws = jax.random.uniform(jax.random.fold_in(jax.random.fold_in(rng, 6), dim), (blocks,), jnp.float32, smallest / len(cuts), largest / len(cuts))
        gain = gain * jnp.repeat(jnp.exp(draws), shape[dim] // blocks).reshape((-1,) + (1,) * (len(shape) - 1 - dim))
    return gain


def assign_block(rng, own, number, rows, number_of, top, bound, skew):
    sequence = jax.random.permutation(rng, number_of)
    packed, common = portions_of(number_of, rows * top, bound, skew, True), portions_of(number_of, rows * top, bound, skew, False)
    places = jnp.arange(number_of)

    def named(sizes, rotation):
        used = int((sizes > 0).sum())
        fixed = max(1, used // 4)
        shifted = fixed + (places - fixed + rotation * (used - fixed)) % max(1, number_of - fixed)
        return jnp.zeros((number_of,), jnp.int32).at[sequence[jnp.where(places < fixed, places, shifted)]].set(jnp.asarray(sizes, jnp.int32))

    sizes = jnp.where(number % 4 == 0, named(packed, number // 4), named(common, number - number // 4 - 1))
    mixed = jax.random.permutation(jax.random.fold_in(own, 3), number_of)
    source_of, taker = mixed[0:number_of // 2 * 2:2], mixed[1:number_of // 2 * 2:2]
    slack = jnp.minimum(sizes[source_of] - 1, bound - sizes[taker]) // 2
    slack = jnp.where((source_of == sequence[0]) | (taker == sequence[0]) | (sizes[taker] == 0), 0, jnp.maximum(slack, 0))
    shifted = jax.random.randint(jax.random.fold_in(own, 4), (number_of // 2,), 0, 1 << 20) % (slack + 1)
    sizes = sizes.at[source_of].add(-shifted).at[taker].add(shifted)
    labels = jnp.searchsorted(jnp.cumsum(sizes), jnp.arange(rows * top), side="right").astype(jnp.int32)
    table = labels.reshape(top, rows).T
    table = table[jax.random.permutation(jax.random.fold_in(own, 1), rows)]
    rotation = jax.random.randint(jax.random.fold_in(own, 2), (rows, 1), 0, top)
    return jnp.take_along_axis(table, (jnp.arange(top)[None, :] + rotation) % top, axis=1)


def portions_of(number_of, total, most, skew, full):
    loads = [(1 << 20) // math.isqrt(rank ** skew) + 1 for rank in range(1, number_of + 1)]
    largest = most if full else min(most, max(-(-total // number_of), total * loads[0] // sum(loads)))
    least = 1 if total - largest >= number_of - 1 else 0
    holding, surplus = [largest] + [least] * (number_of - 1), total - largest - least * (number_of - 1)
    while surplus > 0:
        movable = [i for i in range(1, number_of) if holding[i] < largest] or [i for i in range(1, number_of) if holding[i] < most]
        pool, left = sum([loads[i] for i in movable]), surplus
        for i in movable:
            more = min(most - holding[i], max(1, left * loads[i] // pool), surplus)
            holding[i] = holding[i] + more
            surplus = surplus - more
    return np.array(holding)


def scatter_about(own_key, extent, scale, most, pieces=(), kind=jnp.bfloat16):
    factor_of = shard_levels(own_key, extent, pieces, -0.22, 0.18) if pieces else 1.0
    entries = jax.random.normal(own_key, extent, jnp.float32) * scale * factor_of
    return jnp.minimum(jnp.maximum(entries, -most), most).astype(kind)


def setup_inputs(seed: int = 0) -> dict:
    key_of = jax.random.split(jax.random.key(seed), 5)
    visual = scatter_about(key_of[0], (VISUAL, DV), 1.0, 6.0, ((0, 32),))
    text_queries = draw_text_queries(jax.random.fold_in(key_of[4], 71), 0)
    kv_weight = scatter_about(key_of[2], (DV, 2 * KV_HEADS * HEAD_DIM), DV ** -0.5, 0.09375)
    placement_keys = jax.random.split(jax.random.fold_in(key_of[3], 1), (BLOCKS * DEVICES) // BLOCKS)
    placement_turns = jax.random.permutation(jax.random.fold_in(key_of[3], 3), (BLOCKS * DEVICES) // BLOCKS)
    placement = jax.vmap(lambda own, number: assign_block(jax.random.fold_in(key_of[3], 2), own, number, BLOCKS, DEVICES, 1, PER_PAIR, 2))(placement_keys, placement_turns).reshape((BLOCKS * DEVICES, 1))
    return dict(visual=visual, text_queries=text_queries, kv_weight=kv_weight, placement=placement)


def reference(visual, text_queries, kv_weight, placement):
    devices = N_GRP * N_BLK
    group = HEADS // KV_HEADS
    width = 2 * KV_HEADS * HEAD_DIM
    kv = jnp.dot(visual, kv_weight, preferred_element_type=jnp.float32)
    flat_blocks = kv.reshape(devices * BLOCKS, BLOCK_ROWS * width)
    owner = placement.reshape(devices, BLOCKS).astype(jnp.int32)
    index = jnp.arange(BLOCKS, dtype=jnp.int32)
    earlier = (owner[:, :, None] == owner[:, None, :]) & (index[None, None, :] < index[None, :, None])
    rank = jnp.sum(earlier.astype(jnp.int32), axis=2, dtype=jnp.int32)
    source = jnp.arange(devices, dtype=jnp.int32)[:, None]
    slot = owner * (devices * PER_PAIR) + source * PER_PAIR + rank
    span = N_BLK * devices * PER_PAIR
    scale = HEAD_DIM ** -0.5

    def segment(seg):
        local = slot - seg * span
        inside = (local >= 0) & (local < span)
        target = jnp.where(inside, local, span).reshape(-1).astype(jnp.int32)
        buffer = jnp.zeros((span, BLOCK_ROWS * width), jnp.float32).at[target].set(flat_blocks, mode="drop")
        marks = jnp.zeros((span, BLOCK_ROWS), jnp.float32).at[target].set(1.0, mode="drop")
        keys_all = buffer.reshape(span * BLOCK_ROWS, width)
        valid = marks.reshape(-1) > 0.5
        key_heads = keys_all[:, :KV_HEADS * HEAD_DIM].reshape(-1, KV_HEADS, HEAD_DIM)
        value_heads = keys_all[:, KV_HEADS * HEAD_DIM:].reshape(-1, KV_HEADS, HEAD_DIM)
        rows = lax.dynamic_slice_in_dim(text_queries, seg * N_BLK * QROWS, N_BLK * QROWS, 0)
        query_heads = rows.reshape(-1, KV_HEADS, group, HEAD_DIM)
        scores = jnp.einsum("rgjd,kgd->rgjk", query_heads, key_heads, precision=lax.Precision.HIGHEST) * scale
        scores = jnp.where(valid[None, None, None, :], scores, -1e30)
        weights = jax.nn.softmax(scores, axis=-1)
        result = jnp.einsum("rgjk,kgd->rgjd", weights, value_heads, precision=lax.Precision.HIGHEST)
        return result.reshape(N_BLK * QROWS, HEADS * HEAD_DIM)

    results = lax.map(segment, jnp.arange(N_GRP, dtype=jnp.int32))
    return results.reshape(TEXT, HEADS * HEAD_DIM)
```

```python
import functools
import math

import jax
import jax.numpy as jnp
from jax import lax
from jax.experimental import pallas as pl
from jax.experimental.pallas import tpu as pltpu
from jax.sharding import PartitionSpec as P

HEADS = 28
KV_HEADS = 4
MESH = pl.DeviceIdType.MESH
F32 = jnp.float32
BF16 = jnp.bfloat16
NT = (((1,), (1,)), ((), ()))


def dot(a, b):
    return jnp.dot(a, b, preferred_element_type=F32)


def split2(x):
    hi = x.astype(BF16)
    return hi, (x - hi.astype(F32)).astype(BF16)


def kernel(
    n_grp, n_blk, per_seg, group, dim,
    visual_hbm, query_hbm, weight_hbm, place_ref,
    out_ref,
    visual, weight, kv, outgoing, arrived, queries, index_v, index_s,
    counts_out, counts_in, bias, kcat, v_t, scores, probs,
    stats_out, stats_in, partial, partial_in,
    load_sem, weight_sem, query_load_sem, index_sem,
    query_send, query_recv, count_send, count_recv,
    kv_send, kv_recv, stat_send, stat_recv, part_send, part_recv,
):
    me_g = lax.axis_index("grp")
    me_b = lax.axis_index("blk")
    rows = query_hbm.shape[0]
    n_rows = visual.shape[0]
    blocks = place_ref.shape[0]
    block_rows = n_rows // blocks
    seg_rows = per_seg * block_rows
    lanes = n_blk * rows
    keys = n_grp * seg_rows
    slots = n_grp * per_seg
    heads = KV_HEADS
    wide = group * dim
    scale = dim ** (-0.5) * math.log2(math.e)
    tile = load_rows(n_rows)
    tiles = n_rows // tile

    def weight_loads(h):
        return [
            pltpu.make_async_copy(
                weight_hbm.at[:, pl.ds((half * heads + h) * dim, dim)],
                weight.at[h % 2, :, pl.ds(half * dim, dim)],
                weight_sem.at[h % 2, half],
            )
            for half in range(2)
        ]

    def visual_load(i):
        at = pl.ds(pl.multiple_of(i * tile, tile), tile)
        return pltpu.make_async_copy(visual_hbm.at[at, :], visual.at[at, :], load_sem.at[i])

    query_load = pltpu.make_async_copy(query_hbm, queries.at[me_b], query_load_sem)
    for copy in weight_loads(0):
        copy.start()
    visual_load(0).start()
    query_load.start()
    for i in range(1, tiles):
        visual_load(i).start()

    barrier = pltpu.get_barrier_semaphore()
    for d in range(1, n_grp):
        pl.semaphore_signal(
            barrier, inc=1, device_id={"grp": lax.rem(me_g + d, n_grp)}, device_id_type=MESH
        )
    for e in range(1, n_blk):
        pl.semaphore_signal(
            barrier, inc=1, device_id={"blk": lax.rem(me_b + e, n_blk)}, device_id_type=MESH
        )

    owner = place_ref[...]
    seg = jnp.zeros_like(owner)
    for g in range(1, n_grp):
        seg += (owner >= g * n_blk).astype(jnp.int32)
    block_id = lax.broadcasted_iota(jnp.int32, (blocks, slots), 0)
    slot_id = lax.broadcasted_iota(jnp.int32, (blocks, slots), 1)
    slot_seg = jnp.zeros_like(slot_id)
    for g in range(1, n_grp):
        slot_seg += (slot_id >= g * per_seg).astype(jnp.int32)
    inside = jnp.broadcast_to(seg, (blocks, slots)) == slot_seg
    member = inside.astype(jnp.int32)
    running = member
    shift = 1
    while shift < blocks:
        running += jnp.where(block_id >= shift, pltpu.roll(running, shift, 0), 0)
        shift *= 2
    hit = inside & (running - member == slot_id - slot_seg * per_seg)
    index = jnp.sum(jnp.where(hit, block_id, 0), axis=0, keepdims=True)
    index_v[...] = jnp.broadcast_to(index, index_v.shape)
    index_copy = pltpu.make_async_copy(index_v, index_s, index_sem)
    index_copy.start()
    for d in range(n_grp):
        g = lax.rem(me_g + d, n_grp)
        count = jnp.sum((seg == g).astype(F32), axis=0, keepdims=True) * block_rows
        counts_out[d] = jnp.broadcast_to(count, counts_out.shape[1:])
    counts_in[0] = counts_out[0]

    pl.semaphore_wait(barrier, n_grp + n_blk - 2)

    def query_path(way, hop):
        step = 1 if way == 0 else n_blk - 1
        source = lax.rem(me_b + hop * (n_blk - step), n_blk)
        peer = lax.rem(me_b + step, n_blk)
        if way == 0:
            ok = jnp.logical_and(me_b >= hop, me_b < n_blk - 1)
        else:
            ok = jnp.logical_and(me_b < n_blk - hop, me_b >= 1)
        return source, peer, ok

    def query_copy(way, hop, h):
        source, peer, ok = query_path(way, hop)
        cols = pl.ds(h * wide, wide)
        copy = pltpu.make_async_remote_copy(
            src_ref=queries.at[source, :, cols],
            dst_ref=queries.at[source, :, cols],
            send_sem=query_send.at[way, hop, h],
            recv_sem=query_recv.at[way, hop + 1, h],
            device_id={"blk": peer},
            device_id_type=MESH,
        )
        return copy, ok

    def query_arrival(way, hop, h):
        source = query_path(way, hop)[0]
        at = queries.at[source, :, pl.ds(h * wide, wide)]
        return pltpu.make_async_copy(at, at, query_recv.at[way, hop, h])

    def query_send_on(hop, h):
        for way in range(2):
            copy, ok = query_copy(way, hop, h)

            @pl.when(ok)
            def _(copy=copy, way=way):
                if hop > 0:
                    query_arrival(way, hop, h).wait()
                copy.start()

    def query_wait(h):
        for way in range(2):
            for hop in range(1, n_blk):
                @pl.when(me_b == (n_blk - 1 if way == 0 else 0))
                def _(copy=query_arrival(way, hop, h)):
                    copy.wait()

    relay_points = {}
    first_point = [0, 2, 4, 5]
    for h in range(heads):
        limit = 3 if h == 0 else 3 + 2 * h
        for hop in range(1, n_blk - 1):
            point = min(first_point[min(h, 3)] + (hop - 1) * (2 if h == 0 else 1), limit)
            relay_points.setdefault(point, []).append((hop, h))
    relay_points.setdefault(1, []).append((0, 2))
    relay_points.setdefault(3, []).append((0, 3))

    def relay(point):
        for hop, h in sorted(relay_points.get(point, []), key=lambda t: (t[1], t[0])):
            query_send_on(hop, h)

    def kv_copy(unit, d):
        return pltpu.make_async_remote_copy(
            src_ref=outgoing.at[unit, d - 1],
            dst_ref=arrived.at[unit, d],
            send_sem=kv_send.at[unit, d],
            recv_sem=kv_recv.at[unit, d],
            device_id={"grp": lax.rem(me_g + d, n_grp)},
            device_id_type=MESH,
        )

    def count_copy(d):
        return pltpu.make_async_remote_copy(
            src_ref=counts_out.at[d],
            dst_ref=counts_in.at[d],
            send_sem=count_send.at[d],
            recv_sem=count_recv.at[d],
            device_id={"grp": lax.rem(me_g + d, n_grp)},
            device_id_type=MESH,
        )

    query_load.wait()
    query_send_on(0, 0)
    query_send_on(0, 1)

    for h in range(heads):
        for copy in weight_loads(h):
            copy.wait()

        def project(i, _, h=h):
            if h == 0:
                visual_load(i).wait()
            at = pl.ds(pl.multiple_of(i * tile, tile), tile)
            to = pl.ds(i * (tile // block_rows), tile // block_rows)
            kv[to] = dot(visual[at, :], weight[h % 2]).reshape(-1, block_rows, 2 * dim)
            return 0

        if h == 0:
            for copy in weight_loads(1):
                copy.start()
        lax.fori_loop(0, tiles, project, 0)
        if h + 2 < heads:
            for copy in weight_loads(h + 2):
                copy.start()
        if h == 0:
            index_copy.wait()

        def pack(d, target, place, h=h):
            first = lax.rem(me_g + d, n_grp) * per_seg
            for r in range(per_seg):
                block = index_s[0, first + r]
                both = kv[block]
                to = pl.ds(r * block_rows, block_rows)
                target[2 * h, place, to, :] = both[:, :dim]
                target[2 * h + 1, place, to, :] = both[:, dim:]

        def pack_peer(d, _):
            pack(d, outgoing, d - 1)
            return 0

        lax.fori_loop(1, n_grp, pack_peer, 0)
        for unit in (2 * h, 2 * h + 1):
            for d in range(1, n_grp):
                kv_copy(unit, d).start()
        pack(0, arrived, 0)
        if h == 0:
            for d in range(1, n_grp):
                count_copy(d).start()
        relay(h)

    for d in range(1, n_grp):
        count_copy(d).wait_recv()
    key_id = lax.broadcasted_iota(jnp.int32, (seg_rows, 128), 0).astype(F32)
    for d in range(n_grp):
        bias[d * seg_rows : (d + 1) * seg_rows, :] = jnp.where(
            key_id < counts_in[d][0:1, :], 0.0, -1e30
        )

    def stat_copy(h, e):
        return pltpu.make_async_remote_copy(
            src_ref=stats_out.at[h],
            dst_ref=stats_in.at[h, e],
            send_sem=stat_send.at[h, e],
            recv_sem=stat_recv.at[h, e],
            device_id={"blk": lax.rem(me_b + e, n_blk)},
            device_id_type=MESH,
        )

    def part_copy(h, e):
        peer = lax.rem(me_b + e, n_blk)
        return pltpu.make_async_remote_copy(
            src_ref=partial.at[h, peer],
            dst_ref=partial_in.at[h, e - 1],
            send_sem=part_send.at[h, e],
            recv_sem=part_recv.at[h, e],
            device_id={"blk": peer},
            device_id_type=MESH,
        )

    for h in range(heads):
        query_wait(h)
        for d in range(1, n_grp):
            kv_copy(2 * h, d).wait_recv()
        hi, low = split2(arrived[2 * h].reshape(keys, dim))
        kcat[:, :dim] = hi
        kcat[:, dim:] = low
        stats_out[h] = jnp.zeros_like(stats_out[h])

        def score(j, slot, h=h):
            at = pl.ds(pl.multiple_of((h * group + j) * dim, dim), dim)
            hi, low = split2(queries[:, :, at].reshape(lanes, dim) * scale)
            both = jnp.concatenate(
                [jnp.concatenate([hi, hi], 1), jnp.concatenate([low, low], 1)], 0
            )
            s = lax.dot_general(kcat[...], both, NT, preferred_element_type=F32)
            b = bias[...]
            if lanes > 128:
                b = jnp.concatenate([b] * (lanes // 128), 1)
            s = s[:, :lanes] + s[:, lanes:] + b
            scores[slot] = s
            stats_out[h, 0, pl.ds(j, 1), :] = jnp.max(s, axis=0, keepdims=True)

        def weigh(j, slot, h=h):
            p = jnp.exp2(scores[slot] - stats_out[h, 0, pl.ds(j, 1), :])
            stats_out[h, 1, pl.ds(j, 1), :] = jnp.sum(p, axis=0, keepdims=True)
            hi, low = split2(p)
            probs[j, :, :lanes] = hi
            probs[j, :, lanes:] = low

        score(0, 0)

        def step(i, _):
            score(2 * i + 1, 1)
            weigh(2 * i, 0)
            score(2 * i + 2, 0)
            weigh(2 * i + 1, 1)
            return 0

        pairs = (group - 1) // 2
        lax.fori_loop(0, pairs, step, 0)
        if group % 2 == 0:
            score(group - 1, 1)
        weigh(2 * pairs, 0)
        if group % 2 == 0:
            weigh(group - 1, 1)
        for e in range(1, n_blk):
            stat_copy(h, e).start()
        relay(4 + 2 * h)

        for d in range(1, n_grp):
            kv_copy(2 * h + 1, d).wait_recv()
        hi, low = split2(arrived[2 * h + 1].reshape(keys, dim).T)
        v_t[:dim, :] = hi
        v_t[dim:, :] = low
        for e in range(1, n_blk):
            stat_copy(h, e).wait_recv()
        mine = stats_out[h, 0]
        top = mine
        for e in range(1, n_blk):
            top = jnp.maximum(top, stats_in[h, e, 0])
        factor = jnp.exp2(mine - top)
        whole = stats_out[h, 1] * factor
        for e in range(1, n_blk):
            whole += stats_in[h, e, 1] * jnp.exp2(stats_in[h, e, 0] - top)
        stats_in[h, 0, 0] = factor / whole

        def mix(j, _, h=h):
            o = dot(v_t[...], probs[j])
            o = (o[:dim, :lanes] + o[dim:, :lanes]) + (o[:dim, lanes:] + o[dim:, lanes:])
            o = (o * stats_in[h, 0, 0, pl.ds(j, 1), :]).T
            at = pl.ds(pl.multiple_of(j * dim, dim), dim)
            partial[h, :, :, at] = o.reshape(n_blk, rows, dim)
            return 0

        lax.fori_loop(0, group, mix, 0)
        for e in range(1, n_blk):
            part_copy(h, e).start()
        relay(5 + 2 * h)

    for h in range(heads):
        for e in range(1, n_blk):
            part_copy(h, e).wait_recv()
        total = partial[h, me_b]
        for e in range(1, n_blk):
            total += partial_in[h, e - 1]
        out_ref[:, h * wide : (h + 1) * wide] = total

    for h in range(heads):
        for hop in range(n_blk - 1):
            for way in range(2):
                copy, ok = query_copy(way, hop, h)

                @pl.when(ok)
                def _(copy=copy):
                    copy.wait_send()
        for d in range(1, n_grp):
            kv_copy(2 * h, d).wait_send()
            kv_copy(2 * h + 1, d).wait_send()
        for e in range(1, n_blk):
            stat_copy(h, e).wait_send()
            part_copy(h, e).wait_send()
    for d in range(1, n_grp):
        count_copy(d).wait_send()


def load_rows(n_rows):
    return math.gcd(256, n_rows)


def on_device(n_grp, n_blk, visual, text_queries, kv_weight, placement):
    n_rows, model = visual.shape
    rows, wide = text_queries.shape
    dim = kv_weight.shape[1] // (2 * KV_HEADS)
    group = wide // dim // KV_HEADS
    blocks = placement.shape[0]
    block_rows = n_rows // blocks
    per_pair = max(2, blocks // (n_grp * n_blk) + 1)
    per_seg = n_blk * per_pair
    seg_rows = per_seg * block_rows
    keys = n_grp * seg_rows
    slots = n_grp * per_seg
    lanes = n_blk * rows
    heads = KV_HEADS
    units = 2 * heads
    stat_rows = -(-group // 8) * 8
    tiles = n_rows // load_rows(n_rows)
    any_space = pl.BlockSpec(memory_space=pl.ANY)
    in_vmem = pl.BlockSpec(memory_space=pltpu.VMEM)
    dma = pltpu.SemaphoreType.DMA
    return pl.pallas_call(
        functools.partial(kernel, n_grp, n_blk, per_seg, group, dim),
        name="routed_attention",
        out_shape=jax.ShapeDtypeStruct((rows, wide), F32),
        in_specs=[any_space, any_space, any_space, in_vmem],
        out_specs=in_vmem,
        scratch_shapes=[
            pltpu.VMEM((n_rows, model), BF16),
            pltpu.VMEM((2, model, 2 * dim), BF16),
            pltpu.VMEM((blocks, block_rows, 2 * dim), F32),
            pltpu.VMEM((units, n_grp - 1, seg_rows, dim), F32),
            pltpu.VMEM((units, n_grp, seg_rows, dim), F32),
            pltpu.VMEM((n_blk, rows, wide), F32),
            pltpu.VMEM((8, slots), jnp.int32),
            pltpu.SMEM((8, slots), jnp.int32),
            pltpu.VMEM((n_grp, 8, 128), F32),
            pltpu.VMEM((n_grp, 8, 128), F32),
            pltpu.VMEM((keys, 128), F32),
            pltpu.VMEM((keys, 2 * dim), BF16),
            pltpu.VMEM((2 * dim, keys), BF16),
            pltpu.VMEM((2, keys, lanes), F32),
            pltpu.VMEM((group, keys, 2 * lanes), BF16),
            pltpu.VMEM((heads, 2, stat_rows, lanes), F32),
            pltpu.VMEM((heads, n_blk, 2, stat_rows, lanes), F32),
            pltpu.VMEM((heads, n_blk, rows, group * dim), F32),
            pltpu.VMEM((heads, n_blk - 1, rows, group * dim), F32),
            dma((tiles,)),
            dma((2, 2)),
            dma,
            dma,
            dma((2, n_blk, heads)),
            dma((2, n_blk, heads)),
            dma((n_grp,)),
            dma((n_grp,)),
            dma((units, n_grp)),
            dma((units, n_grp)),
            dma((heads, n_blk)),
            dma((heads, n_blk)),
            dma((heads, n_blk)),
            dma((heads, n_blk)),
        ],
        compiler_params=pltpu.CompilerParams(
            collective_id=0, has_side_effects=True, vmem_limit_bytes=67043328
        ),
    )(visual, text_queries, kv_weight, placement)


def solution(mesh):
    placed = (P(("grp", "blk"), None), P(("grp", "blk"), None), P(), P(("grp", "blk"), None))
    body = functools.partial(on_device, mesh.shape["grp"], mesh.shape["blk"])
    return jax.shard_map(
        body, mesh=mesh, in_specs=placed, out_specs=P(("grp", "blk"), None), check_vma=False
    )
```

```python
import functools
import math

import jax
import jax.numpy as jnp
from jax import lax
from jax.experimental import pallas as pl
from jax.experimental.pallas import tpu as pltpu
from jax.sharding import PartitionSpec as P

HEADS = 28
KV_HEADS = 4
MESH = pl.DeviceIdType.MESH
F32 = jnp.float32
BF16 = jnp.bfloat16
NT = (((1,), (1,)), ((), ()))


def dot(a, b):
    return jnp.dot(a, b, preferred_element_type=F32)


def split2(x):
    hi = x.astype(BF16)
    return hi, (x - hi.astype(F32)).astype(BF16)


def kernel(
    n_grp, n_blk, per_seg, group, dim,
    visual_hbm, query_hbm, weight_hbm, place_ref,
    out_ref,
    visual, weight, kv, outgoing, arrived, queries, index_v, index_s,
    counts_out, counts_in, bias, kcat, v_t, scores, probs,
    stats_out, stats_in, partial, partial_in, summed,
    load_sem, weight_sem, query_load_sem, index_sem,
    query_send, query_recv, count_send, count_recv,
    kv_send, kv_recv, stat_send, stat_recv, part_send, part_recv, chain_send, chain_recv,
):
    me_g = lax.axis_index("grp")
    me_b = lax.axis_index("blk")
    rows = query_hbm.shape[0]
    n_rows = visual.shape[0]
    blocks = place_ref.shape[0]
    block_rows = n_rows // blocks
    seg_rows = per_seg * block_rows
    lanes = n_blk * rows
    keys = n_grp * seg_rows
    slots = n_grp * per_seg
    heads = KV_HEADS
    wide = group * dim
    scale = dim ** (-0.5) * math.log2(math.e)
    tile = load_rows(n_rows)
    tiles = n_rows // tile

    def weight_loads(h):
        return [
            pltpu.make_async_copy(
                weight_hbm.at[:, pl.ds((half * heads + h) * dim, dim)],
                weight.at[h % 2, :, pl.ds(half * dim, dim)],
                weight_sem.at[h % 2, half],
            )
            for half in range(2)
        ]

    def visual_load(i):
        at = pl.ds(pl.multiple_of(i * tile, tile), tile)
        return pltpu.make_async_copy(visual_hbm.at[at, :], visual.at[at, :], load_sem.at[i])

    query_load = pltpu.make_async_copy(query_hbm, queries.at[me_b], query_load_sem)
    for copy in weight_loads(0):
        copy.start()
    visual_load(0).start()
    query_load.start()
    for i in range(1, tiles):
        visual_load(i).start()

    barrier = pltpu.get_barrier_semaphore()
    for d in range(1, n_grp):
        pl.semaphore_signal(
            barrier, inc=1, device_id={"grp": lax.rem(me_g + d, n_grp)}, device_id_type=MESH
        )
    for e in range(1, n_blk):
        pl.semaphore_signal(
            barrier, inc=1, device_id={"blk": lax.rem(me_b + e, n_blk)}, device_id_type=MESH
        )

    owner = place_ref[...]
    seg = jnp.zeros_like(owner)
    for g in range(1, n_grp):
        seg += (owner >= g * n_blk).astype(jnp.int32)
    block_id = lax.broadcasted_iota(jnp.int32, (blocks, slots), 0)
    slot_id = lax.broadcasted_iota(jnp.int32, (blocks, slots), 1)
    slot_seg = jnp.zeros_like(slot_id)
    for g in range(1, n_grp):
        slot_seg += (slot_id >= g * per_seg).astype(jnp.int32)
    inside = jnp.broadcast_to(seg, (blocks, slots)) == slot_seg
    member = inside.astype(jnp.int32)
    running = member
    shift = 1
    while shift < blocks:
        running += jnp.where(block_id >= shift, pltpu.roll(running, shift, 0), 0)
        shift *= 2
    hit = inside & (running - member == slot_id - slot_seg * per_seg)
    index = jnp.sum(jnp.where(hit, block_id, 0), axis=0, keepdims=True)
    index_v[...] = jnp.broadcast_to(index, index_v.shape)
    index_copy = pltpu.make_async_copy(index_v, index_s, index_sem)
    index_copy.start()
    for d in range(n_grp):
        g = lax.rem(me_g + d, n_grp)
        count = jnp.sum((seg == g).astype(F32), axis=0, keepdims=True) * block_rows
        counts_out[d] = jnp.broadcast_to(count, counts_out.shape[1:])
    counts_in[0] = counts_out[0]

    pl.semaphore_wait(barrier, n_grp + n_blk - 2)

    def query_path(way, hop):
        step = 1 if way == 0 else n_blk - 1
        source = lax.rem(me_b + hop * (n_blk - step), n_blk)
        peer = lax.rem(me_b + step, n_blk)
        if way == 0:
            ok = jnp.logical_and(me_b >= hop, me_b < n_blk - 1)
        else:
            ok = jnp.logical_and(me_b < n_blk - hop, me_b >= 1)
        return source, peer, ok

    def query_copy(way, hop, h):
        source, peer, ok = query_path(way, hop)
        cols = pl.ds(h * wide, wide)
        copy = pltpu.make_async_remote_copy(
            src_ref=queries.at[source, :, cols],
            dst_ref=queries.at[source, :, cols],
            send_sem=query_send.at[way, hop, h],
            recv_sem=query_recv.at[way, hop + 1, h],
            device_id={"blk": peer},
            device_id_type=MESH,
        )
        return copy, ok

    def query_arrival(way, hop, h):
        source = query_path(way, hop)[0]
        at = queries.at[source, :, pl.ds(h * wide, wide)]
        return pltpu.make_async_copy(at, at, query_recv.at[way, hop, h])

    def query_send_on(hop, h):
        for way in range(2):
            copy, ok = query_copy(way, hop, h)

            @pl.when(ok)
            def _(copy=copy, way=way):
                if hop > 0:
                    query_arrival(way, hop, h).wait()
                copy.start()

    def query_wait(h):
        for way in range(2):
            for hop in range(1, n_blk):
                @pl.when(me_b == (n_blk - 1 if way == 0 else 0))
                def _(copy=query_arrival(way, hop, h)):
                    copy.wait()

    relay_points = {}
    first_point = [0, 2, 4, 5]
    for h in range(heads):
        limit = 3 if h == 0 else 3 + 2 * h
        for hop in range(1, n_blk - 1):
            point = min(first_point[min(h, 3)] + (hop - 1) * (2 if h == 0 else 1), limit)
            relay_points.setdefault(point, []).append((hop, h))
    relay_points.setdefault(1, []).append((0, 2))
    relay_points.setdefault(3, []).append((0, 3))

    def relay(point):
        for hop, h in sorted(relay_points.get(point, []), key=lambda t: (t[1], t[0])):
            query_send_on(hop, h)

    def kv_copy(unit, d):
        return pltpu.make_async_remote_copy(
            src_ref=outgoing.at[unit, d - 1],
            dst_ref=arrived.at[unit, d],
            send_sem=kv_send.at[unit, d],
            recv_sem=kv_recv.at[unit, d],
            device_id={"grp": lax.rem(me_g + d, n_grp)},
            device_id_type=MESH,
        )

    def count_copy(d):
        return pltpu.make_async_remote_copy(
            src_ref=counts_out.at[d],
            dst_ref=counts_in.at[d],
            send_sem=count_send.at[d],
            recv_sem=count_recv.at[d],
            device_id={"grp": lax.rem(me_g + d, n_grp)},
            device_id_type=MESH,
        )

    query_load.wait()
    query_send_on(0, 0)
    query_send_on(0, 1)

    for h in range(heads):
        for copy in weight_loads(h):
            copy.wait()

        def project(i, _, h=h):
            if h == 0:
                visual_load(i).wait()
            at = pl.ds(pl.multiple_of(i * tile, tile), tile)
            to = pl.ds(i * (tile // block_rows), tile // block_rows)
            kv[to] = dot(visual[at, :], weight[h % 2]).reshape(-1, block_rows, 2 * dim)
            return 0

        if h == 0:
            for copy in weight_loads(1):
                copy.start()
        lax.fori_loop(0, tiles, project, 0)
        if h + 2 < heads:
            for copy in weight_loads(h + 2):
                copy.start()
        if h == 0:
            index_copy.wait()

        def pack(d, target, place, h=h):
            first = lax.rem(me_g + d, n_grp) * per_seg
            for r in range(per_seg):
                block = index_s[0, first + r]
                both = kv[block]
                to = pl.ds(r * block_rows, block_rows)
                target[2 * h, place, to, :] = both[:, :dim]
                target[2 * h + 1, place, to, :] = both[:, dim:]

        def pack_peer(d, _):
            pack(d, outgoing, d - 1)
            return 0

        lax.fori_loop(1, n_grp, pack_peer, 0)
        for unit in (2 * h, 2 * h + 1):
            for d in range(1, n_grp):
                kv_copy(unit, d).start()
        pack(0, arrived, 0)
        if h == 0:
            for d in range(1, n_grp):
                count_copy(d).start()
        relay(h)

    for d in range(1, n_grp):
        count_copy(d).wait_recv()
    key_id = lax.broadcasted_iota(jnp.int32, (seg_rows, 128), 0).astype(F32)
    for d in range(n_grp):
        bias[d * seg_rows : (d + 1) * seg_rows, :] = jnp.where(
            key_id < counts_in[d][0:1, :], 0.0, -1e30
        )

    def stat_copy(h, e):
        return pltpu.make_async_remote_copy(
            src_ref=stats_out.at[h],
            dst_ref=stats_in.at[h, e],
            send_sem=stat_send.at[h, e],
            recv_sem=stat_recv.at[h, e],
            device_id={"blk": lax.rem(me_b + e, n_blk)},
            device_id_type=MESH,
        )

    cuts = part_cuts(group)
    parts = len(cuts) - 1

    def part_copy(part, e):
        peer = lax.rem(me_b + e, n_blk)
        cols = pl.ds(cuts[part] * dim, (cuts[part + 1] - cuts[part]) * dim)
        return pltpu.make_async_remote_copy(
            src_ref=partial.at[heads - 1, peer, :, cols],
            dst_ref=partial_in.at[e - 1, :, cols],
            send_sem=part_send.at[part, e],
            recv_sem=part_recv.at[part, e],
            device_id={"blk": peer},
            device_id_type=MESH,
        )

    def chain_copy(h, way, dest):
        step = 1 if way == 0 else n_blk - 1
        return pltpu.make_async_remote_copy(
            src_ref=partial.at[h, dest],
            dst_ref=summed.at[h, dest + 1 - way],
            send_sem=chain_send.at[h, way, dest],
            recv_sem=chain_recv.at[h, way, dest],
            device_id={"blk": lax.rem(me_b + step, n_blk)},
            device_id_type=MESH,
        )

    def chain_dests(way, stage):
        far = range(n_blk - 1, stage, -1)
        return [d if way == 0 else n_blk - 1 - d for d in far]

    def at_stage(way, stage):
        return pl.when(me_b == (stage if way == 0 else n_blk - 1 - stage))

    def chain(h, stage):
        for way in range(2):
            @at_stage(way, stage)
            def _(way=way):
                for dest in chain_dests(way, stage):
                    copy = chain_copy(h, way, dest)
                    if stage > 0:
                        copy.wait_recv()
                        partial[h, dest] += summed[h, dest + 1 - way]
                    copy.start()

    def chain_end(h):
        cols = slice(h * wide, (h + 1) * wide)
        out_ref[:, cols] = partial[h, me_b]
        for way in range(2):
            @pl.when(me_b > 0 if way == 0 else me_b < n_blk - 1)
            def _(way=way):
                chain_copy(h, way, me_b).wait_recv()
                out_ref[:, cols] += summed[h, me_b + 1 - way]

    def chains(point):
        for h in range(heads - 1):
            if point == 5 + 2 * h:
                chain(h, 0)
            elif point == 6 + 2 * h:
                for stage in range(1, min(2, n_blk - 1)):
                    chain(h, stage)
            elif point == 7 + 2 * h:
                for stage in range(2, n_blk - 1):
                    chain(h, stage)
            elif point == 8 + 2 * h:
                chain_end(h)

    for h in range(heads):
        query_wait(h)
        for d in range(1, n_grp):
            kv_copy(2 * h, d).wait_recv()
        hi, low = split2(arrived[2 * h].reshape(keys, dim))
        kcat[:, :dim] = hi
        kcat[:, dim:] = low
        stats_out[h] = jnp.zeros_like(stats_out[h])

        def score(j, slot, h=h):
            at = pl.ds(pl.multiple_of((h * group + j) * dim, dim), dim)
            hi, low = split2(queries[:, :, at].reshape(lanes, dim) * scale)
            both = jnp.concatenate(
                [jnp.concatenate([hi, hi], 1), jnp.concatenate([low, low], 1)], 0
            )
            s = lax.dot_general(kcat[...], both, NT, preferred_element_type=F32)
            b = bias[...]
            if lanes > 128:
                b = jnp.concatenate([b] * (lanes // 128), 1)
            s = s[:, :lanes] + s[:, lanes:] + b
            scores[slot] = s
            stats_out[h, 0, pl.ds(j, 1), :] = jnp.max(s, axis=0, keepdims=True)

        def weigh(j, slot, h=h):
            p = jnp.exp2(scores[slot] - stats_out[h, 0, pl.ds(j, 1), :])
            stats_out[h, 1, pl.ds(j, 1), :] = jnp.sum(p, axis=0, keepdims=True)
            hi, low = split2(p)
            probs[j, :, :lanes] = hi
            probs[j, :, lanes:] = low

        score(0, 0)

        def step(i, _):
            score(2 * i + 1, 1)
            weigh(2 * i, 0)
            score(2 * i + 2, 0)
            weigh(2 * i + 1, 1)
            return 0

        pairs = (group - 1) // 2
        lax.fori_loop(0, pairs, step, 0)
        if group % 2 == 0:
            score(group - 1, 1)
        weigh(2 * pairs, 0)
        if group % 2 == 0:
            weigh(group - 1, 1)
        for e in range(1, n_blk):
            stat_copy(h, e).start()
        relay(4 + 2 * h)
        chains(4 + 2 * h)

        for d in range(1, n_grp):
            kv_copy(2 * h + 1, d).wait_recv()
        hi, low = split2(arrived[2 * h + 1].reshape(keys, dim).T)
        v_t[:dim, :] = hi
        v_t[dim:, :] = low
        for e in range(1, n_blk):
            stat_copy(h, e).wait_recv()
        mine = stats_out[h, 0]
        top = mine
        for e in range(1, n_blk):
            top = jnp.maximum(top, stats_in[h, e, 0])
        factor = jnp.exp2(mine - top)
        whole = stats_out[h, 1] * factor
        for e in range(1, n_blk):
            whole += stats_in[h, e, 1] * jnp.exp2(stats_in[h, e, 0] - top)
        stats_in[h, 0, 0] = factor / whole

        def mix(j, h=h):
            o = dot(v_t[...], probs[j])
            o = (o[:dim, :lanes] + o[dim:, :lanes]) + (o[:dim, lanes:] + o[dim:, lanes:])
            o = o * stats_in[h, 0, 0, j : j + 1, :]
            partial[h, :, :, j * dim : (j + 1) * dim] = o.T.reshape(n_blk, rows, dim)

        for part in range(parts):
            for j in range(cuts[part], cuts[part + 1]):
                mix(j)
            if h == heads - 1:
                for e in range(1, n_blk):
                    part_copy(part, e).start()
        relay(5 + 2 * h)
        chains(5 + 2 * h)

    for point in range(4 + 2 * heads, 7 + 2 * heads):
        chains(point)
    for part in range(parts):
        for e in range(1, n_blk):
            part_copy(part, e).wait_recv()
        cols = slice(cuts[part] * dim, cuts[part + 1] * dim)
        total = partial[heads - 1, me_b, :, cols]
        for e in range(1, n_blk):
            total += partial_in[e - 1, :, cols]
        first = (heads - 1) * wide
        out_ref[:, first + cols.start : first + cols.stop] = total

    for h in range(heads - 1):
        for stage in range(n_blk - 1):
            for way in range(2):
                @at_stage(way, stage)
                def _(way=way):
                    for dest in chain_dests(way, stage):
                        chain_copy(h, way, dest).wait_send()
    for part in range(parts):
        for e in range(1, n_blk):
            part_copy(part, e).wait_send()
    for h in range(heads):
        for hop in range(n_blk - 1):
            for way in range(2):
                copy, ok = query_copy(way, hop, h)

                @pl.when(ok)
                def _(copy=copy):
                    copy.wait_send()
        for d in range(1, n_grp):
            kv_copy(2 * h, d).wait_send()
            kv_copy(2 * h + 1, d).wait_send()
        for e in range(1, n_blk):
            stat_copy(h, e).wait_send()
    for d in range(1, n_grp):
        count_copy(d).wait_send()


def part_cuts(group):
    return sorted({0, min(2, group), min(4, group), group})


def load_rows(n_rows):
    return math.gcd(256, n_rows)


def on_device(n_grp, n_blk, visual, text_queries, kv_weight, placement):
    n_rows, model = visual.shape
    rows, wide = text_queries.shape
    dim = kv_weight.shape[1] // (2 * KV_HEADS)
    group = wide // dim // KV_HEADS
    blocks = placement.shape[0]
    block_rows = n_rows // blocks
    per_pair = max(2, blocks // (n_grp * n_blk) + 1)
    per_seg = n_blk * per_pair
    seg_rows = per_seg * block_rows
    keys = n_grp * seg_rows
    slots = n_grp * per_seg
    lanes = n_blk * rows
    heads = KV_HEADS
    units = 2 * heads
    stat_rows = -(-group // 8) * 8
    tiles = n_rows // load_rows(n_rows)
    parts = len(part_cuts(group)) - 1
    any_space = pl.BlockSpec(memory_space=pl.ANY)
    in_vmem = pl.BlockSpec(memory_space=pltpu.VMEM)
    dma = pltpu.SemaphoreType.DMA
    return pl.pallas_call(
        functools.partial(kernel, n_grp, n_blk, per_seg, group, dim),
        name="routed_attention",
        out_shape=jax.ShapeDtypeStruct((rows, wide), F32),
        in_specs=[any_space, any_space, any_space, in_vmem],
        out_specs=in_vmem,
        scratch_shapes=[
            pltpu.VMEM((n_rows, model), BF16),
            pltpu.VMEM((2, model, 2 * dim), BF16),
            pltpu.VMEM((blocks, block_rows, 2 * dim), F32),
            pltpu.VMEM((units, n_grp - 1, seg_rows, dim), F32),
            pltpu.VMEM((units, n_grp, seg_rows, dim), F32),
            pltpu.VMEM((n_blk, rows, wide), F32),
            pltpu.VMEM((8, slots), jnp.int32),
            pltpu.SMEM((8, slots), jnp.int32),
            pltpu.VMEM((n_grp, 8, 128), F32),
            pltpu.VMEM((n_grp, 8, 128), F32),
            pltpu.VMEM((keys, 128), F32),
            pltpu.VMEM((keys, 2 * dim), BF16),
            pltpu.VMEM((2 * dim, keys), BF16),
            pltpu.VMEM((2, keys, lanes), F32),
            pltpu.VMEM((group, keys, 2 * lanes), BF16),
            pltpu.VMEM((heads, 2, stat_rows, lanes), F32),
            pltpu.VMEM((heads, n_blk, 2, stat_rows, lanes), F32),
            pltpu.VMEM((heads, n_blk, rows, group * dim), F32),
            pltpu.VMEM((n_blk - 1, rows, group * dim), F32),
            pltpu.VMEM((heads - 1, n_blk + 1, rows, group * dim), F32),
            dma((tiles,)),
            dma((2, 2)),
            dma,
            dma,
            dma((2, n_blk, heads)),
            dma((2, n_blk, heads)),
            dma((n_grp,)),
            dma((n_grp,)),
            dma((units, n_grp)),
            dma((units, n_grp)),
            dma((heads, n_blk)),
            dma((heads, n_blk)),
            dma((parts, n_blk)),
            dma((parts, n_blk)),
            dma((heads - 1, 2, n_blk)),
            dma((heads - 1, 2, n_blk)),
        ],
        compiler_params=pltpu.CompilerParams(
            collective_id=0, has_side_effects=True, vmem_limit_bytes=67043328
        ),
    )(visual, text_queries, kv_weight, placement)


def solution(mesh):
    placed = (P(("grp", "blk"), None), P(("grp", "blk"), None), P(), P(("grp", "blk"), None))
    body = functools.partial(on_device, mesh.shape["grp"], mesh.shape["blk"])
    return jax.shard_map(
        body, mesh=mesh, in_specs=placed, out_specs=P(("grp", "blk"), None), check_vma=False
    )
```

```python
import functools
import math

import jax
import jax.numpy as jnp
from jax import lax
from jax.experimental import pallas as pl
from jax.experimental.pallas import tpu as pltpu
from jax.sharding import PartitionSpec as P

HEADS = 28
CHAINED = 3
KV_HEADS = 4
MESH = pl.DeviceIdType.MESH
F32 = jnp.float32
BF16 = jnp.bfloat16
NT = (((1,), (1,)), ((), ()))


def dot(a, b):
    return jnp.dot(a, b, preferred_element_type=F32)


def split2(x):
    hi = x.astype(BF16)
    return hi, (x - hi.astype(F32)).astype(BF16)


def kernel(
    n_grp, n_blk, per_seg, group, dim,
    visual_hbm, query_hbm, weight_hbm, place_hbm,
    out_ref,
    place_ref, visual, weight, kv, outgoing, arrived, queries, index_v, index_s,
    counts_out, counts_in, bias, kcat, v_t, scores, probs,
    stats_out, stats_in, mixing, partial, partial_in, summed,
    load_sem, weight_sem, query_load_sem, place_sem, index_sem,
    query_send, query_recv, count_send, count_recv,
    kv_send, kv_recv, stat_send, stat_recv, part_send, part_recv, chain_send, chain_recv,
):
    me_g = lax.axis_index("grp")
    me_b = lax.axis_index("blk")
    rows = query_hbm.shape[0]
    n_rows = visual.shape[0]
    blocks = place_ref.shape[1]
    block_rows = n_rows // blocks
    seg_rows = per_seg * block_rows
    lanes = n_blk * rows
    keys = n_grp * seg_rows
    slots = n_grp * per_seg
    heads = KV_HEADS
    wide = group * dim
    scale = dim ** (-0.5) * math.log2(math.e)
    tile = load_rows(n_rows)
    tiles = n_rows // tile

    def weight_loads(h):
        return [
            pltpu.make_async_copy(
                weight_hbm.at[:, pl.ds((half * heads + h) * dim, dim)],
                weight.at[h % 2, :, pl.ds(half * dim, dim)],
                weight_sem.at[h % 2, half],
            )
            for half in range(2)
        ]

    def visual_load(i):
        at = pl.ds(pl.multiple_of(i * tile, tile), tile)
        return pltpu.make_async_copy(visual_hbm.at[at, :], visual.at[at, :], load_sem.at[i])

    query_load = pltpu.make_async_copy(query_hbm, queries.at[me_b], query_load_sem)
    place_load = pltpu.make_async_copy(place_hbm, place_ref, place_sem)
    place_load.start()
    for copy in weight_loads(0):
        copy.start()
    visual_load(0).start()
    query_load.start()
    for i in range(1, tiles):
        visual_load(i).start()

    barrier = pltpu.get_barrier_semaphore()
    for d in range(1, n_grp):
        pl.semaphore_signal(
            barrier, inc=1, device_id={"grp": lax.rem(me_g + d, n_grp)}, device_id_type=MESH
        )
    for e in range(1, n_blk):
        pl.semaphore_signal(
            barrier, inc=1, device_id={"blk": lax.rem(me_b + e, n_blk)}, device_id_type=MESH
        )

    place_load.wait()
    owner = jnp.broadcast_to(place_ref[...], (slots, blocks)).T
    seg = jnp.zeros_like(owner)
    for g in range(1, n_grp):
        seg += (owner >= g * n_blk).astype(jnp.int32)
    block_id = lax.broadcasted_iota(jnp.int32, (blocks, slots), 0)
    slot_id = lax.broadcasted_iota(jnp.int32, (blocks, slots), 1)
    slot_seg = jnp.zeros_like(slot_id)
    for g in range(1, n_grp):
        slot_seg += (slot_id >= g * per_seg).astype(jnp.int32)
    inside = seg == slot_seg
    member = inside.astype(jnp.int32)
    running = member
    shift = 1
    while shift < blocks:
        running += jnp.where(block_id >= shift, pltpu.roll(running, shift, 0), 0)
        shift *= 2
    hit = inside & (running - member == slot_id - slot_seg * per_seg)
    index = jnp.sum(jnp.where(hit, block_id, 0), axis=0, keepdims=True)
    index_v[...] = jnp.broadcast_to(index, index_v.shape)
    index_copy = pltpu.make_async_copy(index_v, index_s, index_sem)
    index_copy.start()
    for d in range(n_grp):
        g = lax.rem(me_g + d, n_grp)
        count = jnp.sum((seg[:, :128] == g).astype(F32), axis=0, keepdims=True) * block_rows
        counts_out[d] = jnp.broadcast_to(count, counts_out.shape[1:])
    counts_in[0] = counts_out[0]

    def query_path(way, hop):
        step = 1 if way == 0 else n_blk - 1
        source = lax.rem(me_b + hop * (n_blk - step), n_blk)
        peer = lax.rem(me_b + step, n_blk)
        if way == 0:
            ok = jnp.logical_and(me_b >= hop, me_b < n_blk - 1)
        else:
            ok = jnp.logical_and(me_b < n_blk - hop, me_b >= 1)
        return source, peer, ok

    def query_copy(way, hop, h):
        source, peer, ok = query_path(way, hop)
        cols = pl.ds(h * wide, wide)
        copy = pltpu.make_async_remote_copy(
            src_ref=queries.at[source, :, cols],
            dst_ref=queries.at[source, :, cols],
            send_sem=query_send.at[way, hop, h],
            recv_sem=query_recv.at[way, hop + 1, h],
            device_id={"blk": peer},
            device_id_type=MESH,
        )
        return copy, ok

    def query_arrival(way, hop, h):
        source = query_path(way, hop)[0]
        at = queries.at[source, :, pl.ds(h * wide, wide)]
        return pltpu.make_async_copy(at, at, query_recv.at[way, hop, h])

    def query_send_on(hop, h):
        for way in range(2):
            copy, ok = query_copy(way, hop, h)

            @pl.when(ok)
            def _(copy=copy, way=way):
                if hop > 0:
                    query_arrival(way, hop, h).wait()
                copy.start()

    def query_wait(h):
        for way in range(2):
            for hop in range(1, n_blk):
                @pl.when(me_b == (n_blk - 1 if way == 0 else 0))
                def _(copy=query_arrival(way, hop, h)):
                    copy.wait()

    relay_points = {}
    first_point = [0, 2, 4, 5]
    for h in range(heads):
        limit = 3 if h == 0 else 3 + 2 * h
        for hop in range(1, n_blk - 1):
            point = min(first_point[min(h, 3)] + (hop - 1) * (2 if h == 0 else 1), limit)
            relay_points.setdefault(point, []).append((hop, h))
    relay_points.setdefault(1, []).append((0, 2))
    relay_points.setdefault(3, []).append((0, 3))

    def relay(point):
        for hop, h in sorted(relay_points.get(point, []), key=lambda t: (t[1], t[0])):
            query_send_on(hop, h)

    def kv_copy(unit, d):
        return pltpu.make_async_remote_copy(
            src_ref=outgoing.at[unit, d - 1],
            dst_ref=arrived.at[unit, d],
            send_sem=kv_send.at[unit, d],
            recv_sem=kv_recv.at[unit, d],
            device_id={"grp": lax.rem(me_g + d, n_grp)},
            device_id_type=MESH,
        )

    def count_copy(d):
        return pltpu.make_async_remote_copy(
            src_ref=counts_out.at[d],
            dst_ref=counts_in.at[d],
            send_sem=count_send.at[d],
            recv_sem=count_recv.at[d],
            device_id={"grp": lax.rem(me_g + d, n_grp)},
            device_id_type=MESH,
        )

    for h in range(heads):
        for copy in weight_loads(h):
            copy.wait()

        def project(i, _, h=h):
            if h == 0:
                visual_load(i).wait()
            at = pl.ds(pl.multiple_of(i * tile, tile), tile)
            to = pl.ds(i * (tile // block_rows), tile // block_rows)
            kv[to] = dot(visual[at, :], weight[h % 2]).reshape(-1, block_rows, 2 * dim)
            return 0

        if h == 0:
            for copy in weight_loads(1):
                copy.start()
        lax.fori_loop(0, tiles, project, 0)
        if h + 2 < heads:
            for copy in weight_loads(h + 2):
                copy.start()
        if h == 0:
            index_copy.wait()

        def pack(d, target, place, h=h):
            first = lax.rem(me_g + d, n_grp) * per_seg
            for r in range(per_seg):
                block = index_s[0, first + r]
                both = kv[block]
                to = pl.ds(r * block_rows, block_rows)
                target[2 * h, place, to, :] = both[:, :dim]
                target[2 * h + 1, place, to, :] = both[:, dim:]

        def pack_peer(d, _):
            pack(d, outgoing, d - 1)
            return 0

        lax.fori_loop(1, n_grp, pack_peer, 0)
        if h == 0:
            query_load.wait()
            pl.semaphore_wait(barrier, n_grp + n_blk - 2)
            query_send_on(0, 0)
        for unit in (2 * h, 2 * h + 1):
            for d in range(1, n_grp):
                kv_copy(unit, d).start()
        if h == 0:
            query_send_on(0, 1)
        pack(0, arrived, 0)
        if h == 0:
            for d in range(1, n_grp):
                count_copy(d).start()
        relay(h)

    for d in range(1, n_grp):
        count_copy(d).wait_recv()
    key_id = lax.broadcasted_iota(jnp.int32, (seg_rows, 128), 0).astype(F32)
    for d in range(n_grp):
        bias[d * seg_rows : (d + 1) * seg_rows, :] = jnp.where(
            key_id < counts_in[d][0:1, :], 0.0, -1e30
        )

    def stat_copy(h, e):
        return pltpu.make_async_remote_copy(
            src_ref=stats_out.at[h],
            dst_ref=stats_in.at[h, e],
            send_sem=stat_send.at[h, e],
            recv_sem=stat_recv.at[h, e],
            device_id={"blk": lax.rem(me_b + e, n_blk)},
            device_id_type=MESH,
        )

    cuts = part_cuts(group)
    parts = len(cuts) - 1

    def part_copy(h, part, e):
        peer = lax.rem(me_b + e, n_blk)
        cols = pl.ds(cuts[part] * dim, (cuts[part + 1] - cuts[part]) * dim)
        return pltpu.make_async_remote_copy(
            src_ref=partial.at[h, peer, :, cols],
            dst_ref=partial_in.at[h - CHAINED, e - 1, :, cols],
            send_sem=part_send.at[h - CHAINED, part, e],
            recv_sem=part_recv.at[h - CHAINED, part, e],
            device_id={"blk": peer},
            device_id_type=MESH,
        )

    def head_weights(h):
        for e in range(1, n_blk):
            stat_copy(h, e).wait_recv()
        tops = [stats_out[h, 0]] + [stats_in[h, e, 0] for e in range(1, n_blk)]
        sums = [stats_out[h, 1]] + [stats_in[h, e, 1] for e in range(1, n_blk)]
        top = functools.reduce(jnp.maximum, tops)
        factors = [jnp.exp2(t - top) for t in tops]
        whole = functools.reduce(jnp.add, [s * f for s, f in zip(sums, factors)])
        if h < CHAINED:
            stats_in[h, 0, 0] = factors[0] / whole
        else:
            mixing[h - CHAINED] = jnp.concatenate([f / whole for f in factors], 0).T

    def combine(h):
        mine = mixing[h - CHAINED, pl.ds(pl.multiple_of(me_b * rows, rows), rows), :]
        stat_rows = stats_out.shape[2]
        for part in range(parts):
            for e in range(1, n_blk):
                part_copy(h, part, e).wait_recv()
            for j in range(cuts[part], cuts[part + 1]):
                at = slice(j * dim, (j + 1) * dim)
                total = partial[h, me_b, :, at] * mine[:, j : j + 1]
                for e in range(1, n_blk):
                    col = e * stat_rows + j
                    total += partial_in[h - CHAINED, e - 1, :, at] * mine[:, col : col + 1]
                out_ref[:, h * wide + j * dim : h * wide + (j + 1) * dim] = total

    def chain_copy(h, way, dest):
        step = 1 if way == 0 else n_blk - 1
        return pltpu.make_async_remote_copy(
            src_ref=partial.at[h, dest],
            dst_ref=summed.at[h, dest + 1 - way],
            send_sem=chain_send.at[h, way, dest],
            recv_sem=chain_recv.at[h, way, dest],
            device_id={"blk": lax.rem(me_b + step, n_blk)},
            device_id_type=MESH,
        )

    def chain_dests(way, stage):
        far = range(n_blk - 1, stage, -1)
        return [d if way == 0 else n_blk - 1 - d for d in far]

    def at_stage(way, stage):
        return pl.when(me_b == (stage if way == 0 else n_blk - 1 - stage))

    def chain(h, stage):
        for way in range(2):
            @at_stage(way, stage)
            def _(way=way):
                for dest in chain_dests(way, stage):
                    copy = chain_copy(h, way, dest)
                    if stage > 0:
                        copy.wait_recv()
                        partial[h, dest] += summed[h, dest + 1 - way]
                    copy.start()

    def chain_end(h):
        cols = slice(h * wide, (h + 1) * wide)
        out_ref[:, cols] = partial[h, me_b]
        for way in range(2):
            @pl.when(me_b > 0 if way == 0 else me_b < n_blk - 1)
            def _(way=way):
                chain_copy(h, way, me_b).wait_recv()
                out_ref[:, cols] += summed[h, me_b + 1 - way]

    def chains(point):
        for h in range(CHAINED):
            if point == 5 + 2 * h:
                chain(h, 0)
            elif point == 6 + 2 * h:
                for stage in range(1, min(2, n_blk - 1)):
                    chain(h, stage)
            elif point == 7 + 2 * h:
                for stage in range(2, n_blk - 1):
                    chain(h, stage)
            elif point == 8 + 2 * h:
                chain_end(h)

    for h in range(heads):
        query_wait(h)
        for d in range(1, n_grp):
            kv_copy(2 * h, d).wait_recv()
        hi, low = split2(arrived[2 * h].reshape(keys, dim))
        kcat[:, :dim] = hi
        kcat[:, dim:] = low
        stats_out[h] = jnp.zeros_like(stats_out[h])

        def score(j, slot, h=h):
            at = pl.ds(pl.multiple_of((h * group + j) * dim, dim), dim)
            hi, low = split2(queries[:, :, at].reshape(lanes, dim) * scale)
            both = jnp.concatenate(
                [jnp.concatenate([hi, hi], 1), jnp.concatenate([low, low], 1)], 0
            )
            s = lax.dot_general(kcat[...], both, NT, preferred_element_type=F32)
            b = bias[...]
            if lanes > 128:
                b = jnp.concatenate([b] * (lanes // 128), 1)
            s = s[:, :lanes] + s[:, lanes:] + b
            scores[slot] = s
            stats_out[h, 0, pl.ds(j, 1), :] = jnp.max(s, axis=0, keepdims=True)

        def weigh(j, slot, h=h):
            p = jnp.exp2(scores[slot] - stats_out[h, 0, pl.ds(j, 1), :])
            stats_out[h, 1, pl.ds(j, 1), :] = jnp.sum(p, axis=0, keepdims=True)
            hi, low = split2(p)
            probs[j, :, :lanes] = hi
            probs[j, :, lanes:] = low

        score(0, 0)

        def step(i, _):
            score(2 * i + 1, 1)
            weigh(2 * i, 0)
            score(2 * i + 2, 0)
            weigh(2 * i + 1, 1)
            return 0

        pairs = (group - 1) // 2
        lax.fori_loop(0, pairs, step, 0)
        if group % 2 == 0:
            score(group - 1, 1)
        weigh(2 * pairs, 0)
        if group % 2 == 0:
            weigh(group - 1, 1)
        for e in range(1, n_blk):
            stat_copy(h, e).start()
        relay(4 + 2 * h)
        chains(4 + 2 * h)

        for d in range(1, n_grp):
            kv_copy(2 * h + 1, d).wait_recv()
        hi, low = split2(arrived[2 * h + 1].reshape(keys, dim).T)
        v_t[:dim, :] = hi
        v_t[dim:, :] = low
        if h < CHAINED:
            head_weights(h)

        def mix(j, h=h):
            o = dot(v_t[...], probs[j])
            o = (o[:dim, :lanes] + o[dim:, :lanes]) + (o[:dim, lanes:] + o[dim:, lanes:])
            if h < CHAINED:
                o = o * stats_in[h, 0, 0, j : j + 1, :]
            partial[h, :, :, j * dim : (j + 1) * dim] = o.T.reshape(n_blk, rows, dim)

        for part in range(parts):
            for j in range(cuts[part], cuts[part + 1]):
                mix(j)
            if h >= CHAINED:
                for e in range(1, n_blk):
                    part_copy(h, part, e).start()
        relay(5 + 2 * h)
        chains(5 + 2 * h)
        if h >= CHAINED:
            head_weights(h)
        if h > CHAINED:
            combine(h - 1)

    for point in range(4 + 2 * heads, 7 + 2 * heads):
        chains(point)
    combine(heads - 1)

    for h in range(CHAINED):
        for stage in range(n_blk - 1):
            for way in range(2):
                @at_stage(way, stage)
                def _(way=way):
                    for dest in chain_dests(way, stage):
                        chain_copy(h, way, dest).wait_send()
    for h in range(CHAINED, heads):
        for part in range(parts):
            for e in range(1, n_blk):
                part_copy(h, part, e).wait_send()
    for h in range(heads):
        for hop in range(n_blk - 1):
            for way in range(2):
                copy, ok = query_copy(way, hop, h)

                @pl.when(ok)
                def _(copy=copy):
                    copy.wait_send()
        for d in range(1, n_grp):
            kv_copy(2 * h, d).wait_send()
            kv_copy(2 * h + 1, d).wait_send()
        for e in range(1, n_blk):
            stat_copy(h, e).wait_send()
    for d in range(1, n_grp):
        count_copy(d).wait_send()


def part_cuts(group):
    return sorted({0, min(2, group), min(4, group), group})


def load_rows(n_rows):
    return math.gcd(256, n_rows)


def on_device(n_grp, n_blk, visual, text_queries, kv_weight, placement):
    n_rows, model = visual.shape
    rows, wide = text_queries.shape
    dim = kv_weight.shape[1] // (2 * KV_HEADS)
    group = wide // dim // KV_HEADS
    blocks = placement.shape[0]
    block_rows = n_rows // blocks
    per_pair = max(2, blocks // (n_grp * n_blk) + 1)
    per_seg = n_blk * per_pair
    seg_rows = per_seg * block_rows
    keys = n_grp * seg_rows
    slots = n_grp * per_seg
    lanes = n_blk * rows
    heads = KV_HEADS
    units = 2 * heads
    stat_rows = -(-group // 8) * 8
    tiles = n_rows // load_rows(n_rows)
    parts = len(part_cuts(group)) - 1
    direct = heads - CHAINED
    any_space = pl.BlockSpec(memory_space=pl.ANY)
    in_vmem = pl.BlockSpec(memory_space=pltpu.VMEM)
    dma = pltpu.SemaphoreType.DMA
    return pl.pallas_call(
        functools.partial(kernel, n_grp, n_blk, per_seg, group, dim),
        name="routed_attention",
        out_shape=jax.ShapeDtypeStruct((rows, wide), F32),
        in_specs=[any_space, any_space, any_space, any_space],
        out_specs=in_vmem,
        scratch_shapes=[
            pltpu.VMEM((1, blocks), jnp.int32),
            pltpu.VMEM((n_rows, model), BF16),
            pltpu.VMEM((2, model, 2 * dim), BF16),
            pltpu.VMEM((blocks, block_rows, 2 * dim), F32),
            pltpu.VMEM((units, n_grp - 1, seg_rows, dim), F32),
            pltpu.VMEM((units, n_grp, seg_rows, dim), F32),
            pltpu.VMEM((n_blk, rows, wide), F32),
            pltpu.VMEM((8, slots), jnp.int32),
            pltpu.SMEM((8, slots), jnp.int32),
            pltpu.VMEM((n_grp, 8, 128), F32),
            pltpu.VMEM((n_grp, 8, 128), F32),
            pltpu.VMEM((keys, 128), F32),
            pltpu.VMEM((keys, 2 * dim), BF16),
            pltpu.VMEM((2 * dim, keys), BF16),
            pltpu.VMEM((2, keys, lanes), F32),
            pltpu.VMEM((group, keys, 2 * lanes), BF16),
            pltpu.VMEM((heads, 2, stat_rows, lanes), F32),
            pltpu.VMEM((heads, n_blk, 2, stat_rows, lanes), F32),
            pltpu.VMEM((direct, lanes, n_blk * stat_rows), F32),
            pltpu.VMEM((heads, n_blk, rows, group * dim), F32),
            pltpu.VMEM((direct, n_blk - 1, rows, group * dim), F32),
            pltpu.VMEM((CHAINED, n_blk + 1, rows, group * dim), F32),
            dma((tiles,)),
            dma((2, 2)),
            dma,
            dma,
            dma,
            dma((2, n_blk, heads)),
            dma((2, n_blk, heads)),
            dma((n_grp,)),
            dma((n_grp,)),
            dma((units, n_grp)),
            dma((units, n_grp)),
            dma((heads, n_blk)),
            dma((heads, n_blk)),
            dma((direct, parts, n_blk)),
            dma((direct, parts, n_blk)),
            dma((CHAINED, 2, n_blk)),
            dma((CHAINED, 2, n_blk)),
        ],
        compiler_params=pltpu.CompilerParams(
            collective_id=0, has_side_effects=True, vmem_limit_bytes=67043328
        ),
    )(visual, text_queries, kv_weight, placement.reshape(1, blocks))


def solution(mesh):
    placed = (P(("grp", "blk"), None), P(("grp", "blk"), None), P(), P(("grp", "blk"), None))
    body = functools.partial(on_device, mesh.shape["grp"], mesh.shape["blk"])
    return jax.shard_map(
        body, mesh=mesh, in_specs=placed, out_specs=P(("grp", "blk"), None), check_vma=False
    )
```

```python
import functools
import math

import jax
import jax.numpy as jnp
from jax import lax
from jax.experimental import pallas as pl
from jax.experimental.pallas import tpu as pltpu
from jax.sharding import PartitionSpec as P

HEADS = 28
CHAINED = 3
KV_HEADS = 4
MESH = pl.DeviceIdType.MESH
F32 = jnp.float32
BF16 = jnp.bfloat16
NT = (((1,), (1,)), ((), ()))


def dot(a, b):
    return jnp.dot(a, b, preferred_element_type=F32)


def split2(x):
    hi = x.astype(BF16)
    return hi, (x - hi.astype(F32)).astype(BF16)


def kernel(
    n_grp, n_blk, per_seg, group, dim,
    visual_hbm, query_hbm, weight_hbm, place_hbm,
    out_ref,
    place_ref, visual, weight, kv, outgoing, arrived, queries, index_v, index_s,
    counts_out, counts_in, bias, kcat, v_t, scores, probs,
    stats_out, stats_in, mixing, partial, partial_in, summed,
    load_sem, weight_sem, query_load_sem, place_sem, index_sem,
    query_send, query_recv, count_send, count_recv,
    kv_send, kv_recv, stat_send, stat_recv, part_send, part_recv, chain_send, chain_recv,
):
    me_g = lax.axis_index("grp")
    me_b = lax.axis_index("blk")
    rows = query_hbm.shape[0]
    n_rows = visual.shape[0]
    blocks = place_ref.shape[1]
    block_rows = n_rows // blocks
    seg_rows = per_seg * block_rows
    lanes = n_blk * rows
    keys = n_grp * seg_rows
    slots = n_grp * per_seg
    heads = KV_HEADS
    wide = group * dim
    scale = dim ** (-0.5) * math.log2(math.e)
    tile = load_rows(n_rows)
    tiles = n_rows // tile

    def weight_loads(h):
        return [
            pltpu.make_async_copy(
                weight_hbm.at[:, pl.ds((half * heads + h) * dim, dim)],
                weight.at[h % 2, :, pl.ds(half * dim, dim)],
                weight_sem.at[h % 2, half],
            )
            for half in range(2)
        ]

    def visual_load(i):
        at = pl.ds(pl.multiple_of(i * tile, tile), tile)
        return pltpu.make_async_copy(visual_hbm.at[at, :], visual.at[at, :], load_sem.at[i])

    query_load = pltpu.make_async_copy(query_hbm, queries.at[me_b], query_load_sem)
    place_load = pltpu.make_async_copy(place_hbm, place_ref, place_sem)
    place_load.start()
    for copy in weight_loads(0):
        copy.start()
    visual_load(0).start()
    query_load.start()
    for i in range(1, tiles):
        visual_load(i).start()

    barrier = pltpu.get_barrier_semaphore()
    for d in range(1, n_grp):
        pl.semaphore_signal(
            barrier, inc=1, device_id={"grp": lax.rem(me_g + d, n_grp)}, device_id_type=MESH
        )
    for e in range(1, n_blk):
        pl.semaphore_signal(
            barrier, inc=1, device_id={"blk": lax.rem(me_b + e, n_blk)}, device_id_type=MESH
        )

    place_load.wait()
    owner = jnp.broadcast_to(place_ref[...], (slots, blocks)).T
    seg = jnp.zeros_like(owner)
    for g in range(1, n_grp):
        seg += (owner >= g * n_blk).astype(jnp.int32)
    block_id = lax.broadcasted_iota(jnp.int32, (blocks, slots), 0)
    slot_id = lax.broadcasted_iota(jnp.int32, (blocks, slots), 1)
    slot_seg = jnp.zeros_like(slot_id)
    for g in range(1, n_grp):
        slot_seg += (slot_id >= g * per_seg).astype(jnp.int32)
    inside = seg == slot_seg
    member = inside.astype(jnp.int32)
    running = member
    shift = 1
    while shift < blocks:
        running += jnp.where(block_id >= shift, pltpu.roll(running, shift, 0), 0)
        shift *= 2
    hit = inside & (running - member == slot_id - slot_seg * per_seg)
    index = jnp.sum(jnp.where(hit, block_id, 0), axis=0, keepdims=True)
    index_v[...] = jnp.broadcast_to(index, index_v.shape)
    index_copy = pltpu.make_async_copy(index_v, index_s, index_sem)
    index_copy.start()
    for d in range(n_grp):
        g = lax.rem(me_g + d, n_grp)
        count = jnp.sum((seg[:, :128] == g).astype(F32), axis=0, keepdims=True) * block_rows
        counts_out[d] = jnp.broadcast_to(count, counts_out.shape[1:])
    counts_in[0] = counts_out[0]

    def query_path(way, hop):
        step = 1 if way == 0 else n_blk - 1
        source = lax.rem(me_b + hop * (n_blk - step), n_blk)
        peer = lax.rem(me_b + step, n_blk)
        if way == 0:
            ok = jnp.logical_and(me_b >= hop, me_b < n_blk - 1)
        else:
            ok = jnp.logical_and(me_b < n_blk - hop, me_b >= 1)
        return source, peer, ok

    def query_copy(way, hop, h):
        source, peer, ok = query_path(way, hop)
        cols = pl.ds(h * wide, wide)
        copy = pltpu.make_async_remote_copy(
            src_ref=queries.at[source, :, cols],
            dst_ref=queries.at[source, :, cols],
            send_sem=query_send.at[way, hop, h],
            recv_sem=query_recv.at[way, hop + 1, h],
            device_id={"blk": peer},
            device_id_type=MESH,
        )
        return copy, ok

    def query_arrival(way, hop, h):
        source = query_path(way, hop)[0]
        at = queries.at[source, :, pl.ds(h * wide, wide)]
        return pltpu.make_async_copy(at, at, query_recv.at[way, hop, h])

    def query_send_on(hop, h):
        for way in range(2):
            copy, ok = query_copy(way, hop, h)

            @pl.when(ok)
            def _(copy=copy, way=way):
                if hop > 0:
                    query_arrival(way, hop, h).wait()
                copy.start()

    def query_wait(h):
        for way in range(2):
            for hop in range(1, n_blk):
                @pl.when(me_b == (n_blk - 1 if way == 0 else 0))
                def _(copy=query_arrival(way, hop, h)):
                    copy.wait()

    relay_points = {}
    first_point = [0, 2, 4, 5]
    for h in range(heads):
        limit = 3 if h == 0 else 3 + 2 * h
        for hop in range(1, n_blk - 1):
            point = min(first_point[min(h, 3)] + (hop - 1) * (2 if h == 0 else 1), limit)
            relay_points.setdefault(point, []).append((hop, h))
    relay_points.setdefault(1, []).append((0, 2))
    relay_points.setdefault(3, []).append((0, 3))

    def relay(point):
        for hop, h in sorted(relay_points.get(point, []), key=lambda t: (t[1], t[0])):
            query_send_on(hop, h)

    def kv_copy(unit, d):
        return pltpu.make_async_remote_copy(
            src_ref=outgoing.at[unit, d - 1],
            dst_ref=arrived.at[unit, d],
            send_sem=kv_send.at[unit, d],
            recv_sem=kv_recv.at[unit, d],
            device_id={"grp": lax.rem(me_g + d, n_grp)},
            device_id_type=MESH,
        )

    def count_copy(d):
        return pltpu.make_async_remote_copy(
            src_ref=counts_out.at[d],
            dst_ref=counts_in.at[d],
            send_sem=count_send.at[d],
            recv_sem=count_recv.at[d],
            device_id={"grp": lax.rem(me_g + d, n_grp)},
            device_id_type=MESH,
        )

    for h in range(heads):
        for copy in weight_loads(h):
            copy.wait()

        def project(i, _, h=h):
            if h == 0:
                visual_load(i).wait()
            at = pl.ds(pl.multiple_of(i * tile, tile), tile)
            to = pl.ds(i * (tile // block_rows), tile // block_rows)
            kv[to] = dot(visual[at, :], weight[h % 2]).reshape(-1, block_rows, 2 * dim)
            return 0

        if h == 0:
            for copy in weight_loads(1):
                copy.start()
        lax.fori_loop(0, tiles, project, 0)
        if h + 2 < heads:
            for copy in weight_loads(h + 2):
                copy.start()
        if h == 0:
            index_copy.wait()

        def pack(d, target, place, h=h):
            first = lax.rem(me_g + d, n_grp) * per_seg
            for r in range(per_seg):
                block = index_s[0, first + r]
                both = kv[block]
                to = pl.ds(r * block_rows, block_rows)
                target[2 * h, place, to, :] = both[:, :dim]
                target[2 * h + 1, place, to, :] = both[:, dim:]

        def pack_peer(d, _):
            pack(d, outgoing, d - 1)
            return 0

        lax.fori_loop(1, n_grp, pack_peer, 0)
        if h == 0:
            query_load.wait()
            pl.semaphore_wait(barrier, n_grp + n_blk - 2)
            query_send_on(0, 0)
        for unit in (2 * h, 2 * h + 1):
            for d in range(1, n_grp):
                kv_copy(unit, d).start()
        if h == 0:
            query_send_on(0, 1)
        pack(0, arrived, 0)
        if h == 0:
            for d in range(1, n_grp):
                count_copy(d).start()
        relay(h)

    for d in range(1, n_grp):
        count_copy(d).wait_recv()
    key_id = lax.broadcasted_iota(jnp.int32, (seg_rows, 128), 0).astype(F32)
    for d in range(n_grp):
        bias[d * seg_rows : (d + 1) * seg_rows, :] = jnp.where(
            key_id < counts_in[d][0:1, :], 0.0, -1e30
        )

    def stat_copy(h, e):
        return pltpu.make_async_remote_copy(
            src_ref=stats_out.at[h],
            dst_ref=stats_in.at[h, e],
            send_sem=stat_send.at[h, e],
            recv_sem=stat_recv.at[h, e],
            device_id={"blk": lax.rem(me_b + e, n_blk)},
            device_id_type=MESH,
        )

    cuts = part_cuts(group)
    parts = len(cuts) - 1

    def part_copy(h, part, e):
        peer = lax.rem(me_b + e, n_blk)
        cols = pl.ds(cuts[part] * dim, (cuts[part + 1] - cuts[part]) * dim)
        return pltpu.make_async_remote_copy(
            src_ref=partial.at[h, peer, :, cols],
            dst_ref=partial_in.at[h - CHAINED, e - 1, :, cols],
            send_sem=part_send.at[h - CHAINED, part, e],
            recv_sem=part_recv.at[h - CHAINED, part, e],
            device_id={"blk": peer},
            device_id_type=MESH,
        )

    def head_weights(h):
        for e in range(1, n_blk):
            stat_copy(h, e).wait_recv()
        tops = [stats_out[h, 0]] + [stats_in[h, e, 0] for e in range(1, n_blk)]
        sums = [stats_out[h, 1]] + [stats_in[h, e, 1] for e in range(1, n_blk)]
        top = functools.reduce(jnp.maximum, tops)
        factors = [jnp.exp2(t - top) for t in tops]
        whole = functools.reduce(jnp.add, [s * f for s, f in zip(sums, factors)])
        if h < CHAINED:
            stats_in[h, 0, 0] = factors[0] / whole
        else:
            mixing[h - CHAINED] = jnp.concatenate([f / whole for f in factors], 0).T

    def combine(h):
        mine = mixing[h - CHAINED, pl.ds(pl.multiple_of(me_b * rows, rows), rows), :]
        stat_rows = stats_out.shape[2]
        for part in range(parts):
            for e in range(1, n_blk):
                part_copy(h, part, e).wait_recv()
            for j in range(cuts[part], cuts[part + 1]):
                at = slice(j * dim, (j + 1) * dim)
                total = partial[h, me_b, :, at] * mine[:, j : j + 1]
                for e in range(1, n_blk):
                    col = e * stat_rows + j
                    total += partial_in[h - CHAINED, e - 1, :, at] * mine[:, col : col + 1]
                out_ref[:, h * wide + j * dim : h * wide + (j + 1) * dim] = total

    def chain_copy(h, way, dest):
        step = 1 if way == 0 else n_blk - 1
        return pltpu.make_async_remote_copy(
            src_ref=partial.at[h, dest],
            dst_ref=summed.at[h, dest + 1 - way],
            send_sem=chain_send.at[h, way, dest],
            recv_sem=chain_recv.at[h, way, dest],
            device_id={"blk": lax.rem(me_b + step, n_blk)},
            device_id_type=MESH,
        )

    def chain_dests(way, stage):
        far = range(n_blk - 1, stage, -1)
        return [d if way == 0 else n_blk - 1 - d for d in far]

    def at_stage(way, stage):
        return pl.when(me_b == (stage if way == 0 else n_blk - 1 - stage))

    def chain(h, stage):
        for way in range(2):
            @at_stage(way, stage)
            def _(way=way):
                for dest in chain_dests(way, stage):
                    copy = chain_copy(h, way, dest)
                    if stage > 0:
                        copy.wait_recv()
                        partial[h, dest] += summed[h, dest + 1 - way]
                    copy.start()

    def chain_end(h):
        cols = slice(h * wide, (h + 1) * wide)
        out_ref[:, cols] = partial[h, me_b]
        for way in range(2):
            @pl.when(me_b > 0 if way == 0 else me_b < n_blk - 1)
            def _(way=way):
                chain_copy(h, way, me_b).wait_recv()
                out_ref[:, cols] += summed[h, me_b + 1 - way]

    def chains(point):
        for h in range(CHAINED):
            if point == 5 + 2 * h:
                chain(h, 0)
            elif point == 6 + 2 * h:
                for stage in range(1, min(2, n_blk - 1)):
                    chain(h, stage)
            elif point == 7 + 2 * h:
                for stage in range(2, n_blk - 1):
                    chain(h, stage)
            elif point == 8 + 2 * h:
                chain_end(h)

    for h in range(heads):
        query_wait(h)
        for d in range(1, n_grp):
            kv_copy(2 * h, d).wait_recv()
        hi, low = split2(arrived[2 * h].reshape(keys, dim))
        kcat[:, :dim] = hi
        kcat[:, dim:] = low
        stats_out[h] = jnp.zeros_like(stats_out[h])

        def score(j, slot, h=h):
            at = pl.ds(pl.multiple_of((h * group + j) * dim, dim), dim)
            hi, low = split2(queries[:, :, at].reshape(lanes, dim) * scale)
            both = jnp.concatenate(
                [jnp.concatenate([hi, hi], 1), jnp.concatenate([low, low], 1)], 0
            )
            s = lax.dot_general(kcat[...], both, NT, preferred_element_type=F32)
            b = bias[...]
            if lanes > 128:
                b = jnp.concatenate([b] * (lanes // 128), 1)
            s = s[:, :lanes] + s[:, lanes:] + b
            scores[slot] = s
            stats_out[h, 0, pl.ds(j, 1), :] = jnp.max(s, axis=0, keepdims=True)

        def weigh(j, slot, h=h):
            p = jnp.exp2(scores[slot] - stats_out[h, 0, pl.ds(j, 1), :])
            stats_out[h, 1, pl.ds(j, 1), :] = jnp.sum(p, axis=0, keepdims=True)
            hi, low = split2(p)
            probs[j, :, :lanes] = hi
            probs[j, :, lanes:] = low

        score(0, 0)

        def step(i, _):
            score(2 * i + 1, 1)
            weigh(2 * i, 0)
            score(2 * i + 2, 0)
            weigh(2 * i + 1, 1)
            return 0

        pairs = (group - 1) // 2
        lax.fori_loop(0, pairs, step, 0)
        if group % 2 == 0:
            score(group - 1, 1)
        weigh(2 * pairs, 0)
        if group % 2 == 0:
            weigh(group - 1, 1)
        for e in range(1, n_blk):
            stat_copy(h, e).start()
        relay(4 + 2 * h)
        chains(4 + 2 * h)

        for d in range(1, n_grp):
            kv_copy(2 * h + 1, d).wait_recv()
        hi, low = split2(arrived[2 * h + 1].reshape(keys, dim).T)
        v_t[:dim, :] = hi
        v_t[dim:, :] = low
        if h < CHAINED:
            head_weights(h)

        def mix(j, h=h):
            o = dot(v_t[...], probs[j])
            o = (o[:dim, :lanes] + o[dim:, :lanes]) + (o[:dim, lanes:] + o[dim:, lanes:])
            if h < CHAINED:
                o = o * stats_in[h, 0, 0, j : j + 1, :]
            partial[h, :, :, j * dim : (j + 1) * dim] = o.T.reshape(n_blk, rows, dim)

        for part in range(parts):
            for j in range(cuts[part], cuts[part + 1]):
                mix(j)
            if h >= CHAINED:
                for e in range(1, n_blk):
                    part_copy(h, part, e).start()
        relay(5 + 2 * h)
        chains(5 + 2 * h)
        if h >= CHAINED:
            head_weights(h)
        if h > CHAINED:
            combine(h - 1)

    for point in range(4 + 2 * heads, 7 + 2 * heads):
        chains(point)
    combine(heads - 1)

    for h in range(CHAINED):
        for stage in range(n_blk - 1):
            for way in range(2):
                @at_stage(way, stage)
                def _(way=way):
                    for dest in chain_dests(way, stage):
                        chain_copy(h, way, dest).wait_send()
    for h in range(CHAINED, heads):
        for part in range(parts):
            for e in range(1, n_blk):
                part_copy(h, part, e).wait_send()
    for h in range(heads):
        for hop in range(n_blk - 1):
            for way in range(2):
                copy, ok = query_copy(way, hop, h)

                @pl.when(ok)
                def _(copy=copy):
                    copy.wait_send()
        for d in range(1, n_grp):
            kv_copy(2 * h, d).wait_send()
            kv_copy(2 * h + 1, d).wait_send()
        for e in range(1, n_blk):
            stat_copy(h, e).wait_send()
    for d in range(1, n_grp):
        count_copy(d).wait_send()


def part_cuts(group):
    return sorted({0, min(3, group), group})


def load_rows(n_rows):
    return math.gcd(256, n_rows)


def on_device(n_grp, n_blk, visual, text_queries, kv_weight, placement):
    n_rows, model = visual.shape
    rows, wide = text_queries.shape
    dim = kv_weight.shape[1] // (2 * KV_HEADS)
    group = wide // dim // KV_HEADS
    blocks = placement.shape[0]
    block_rows = n_rows // blocks
    per_pair = max(2, blocks // (n_grp * n_blk) + 1)
    per_seg = n_blk * per_pair
    seg_rows = per_seg * block_rows
    keys = n_grp * seg_rows
    slots = n_grp * per_seg
    lanes = n_blk * rows
    heads = KV_HEADS
    units = 2 * heads
    stat_rows = -(-group // 8) * 8
    tiles = n_rows // load_rows(n_rows)
    parts = len(part_cuts(group)) - 1
    direct = heads - CHAINED
    any_space = pl.BlockSpec(memory_space=pl.ANY)
    in_vmem = pl.BlockSpec(memory_space=pltpu.VMEM)
    dma = pltpu.SemaphoreType.DMA
    return pl.pallas_call(
        functools.partial(kernel, n_grp, n_blk, per_seg, group, dim),
        name="routed_attention",
        out_shape=jax.ShapeDtypeStruct((rows, wide), F32),
        in_specs=[any_space, any_space, any_space, any_space],
        out_specs=in_vmem,
        scratch_shapes=[
            pltpu.VMEM((1, blocks), jnp.int32),
            pltpu.VMEM((n_rows, model), BF16),
            pltpu.VMEM((2, model, 2 * dim), BF16),
            pltpu.VMEM((blocks, block_rows, 2 * dim), F32),
            pltpu.VMEM((units, n_grp - 1, seg_rows, dim), F32),
            pltpu.VMEM((units, n_grp, seg_rows, dim), F32),
            pltpu.VMEM((n_blk, rows, wide), F32),
            pltpu.VMEM((8, slots), jnp.int32),
            pltpu.SMEM((8, slots), jnp.int32),
            pltpu.VMEM((n_grp, 8, 128), F32),
            pltpu.VMEM((n_grp, 8, 128), F32),
            pltpu.VMEM((keys, 128), F32),
            pltpu.VMEM((keys, 2 * dim), BF16),
            pltpu.VMEM((2 * dim, keys), BF16),
            pltpu.VMEM((2, keys, lanes), F32),
            pltpu.VMEM((group, keys, 2 * lanes), BF16),
            pltpu.VMEM((heads, 2, stat_rows, lanes), F32),
            pltpu.VMEM((heads, n_blk, 2, stat_rows, lanes), F32),
            pltpu.VMEM((direct, lanes, n_blk * stat_rows), F32),
            pltpu.VMEM((heads, n_blk, rows, group * dim), F32),
            pltpu.VMEM((direct, n_blk - 1, rows, group * dim), F32),
            pltpu.VMEM((CHAINED, n_blk + 1, rows, group * dim), F32),
            dma((tiles,)),
            dma((2, 2)),
            dma,
            dma,
            dma,
            dma((2, n_blk, heads)),
            dma((2, n_blk, heads)),
            dma((n_grp,)),
            dma((n_grp,)),
            dma((units, n_grp)),
            dma((units, n_grp)),
            dma((heads, n_blk)),
            dma((heads, n_blk)),
            dma((direct, parts, n_blk)),
            dma((direct, parts, n_blk)),
            dma((CHAINED, 2, n_blk)),
            dma((CHAINED, 2, n_blk)),
        ],
        compiler_params=pltpu.CompilerParams(
            collective_id=0, has_side_effects=True, vmem_limit_bytes=67043328
        ),
    )(visual, text_queries, kv_weight, placement.reshape(1, blocks))


def solution(mesh):
    placed = (P(("grp", "blk"), None), P(("grp", "blk"), None), P(), P(("grp", "blk"), None))
    body = functools.partial(on_device, mesh.shape["grp"], mesh.shape["blk"])
    return jax.shard_map(
        body, mesh=mesh, in_specs=placed, out_specs=P(("grp", "blk"), None), check_vma=False
    )
```
